256 devices in a mesh: ga: 2 (over z), aa: 64 (over y, x), ba: 2 (over core).
Axes of the slice: x: 8, y: 8, z: 2, core: 2. Of those that a mesh axis runs over, the one named last changes fastest.
The devices are a block of a 8x8x16 slice.
Arguments:
- images: bfloat16 [16384, 12, 4096], P(('ga', 'aa', 'ba')), parts along dimension 0, may hold values from -6 to 6
- key_projection: bfloat16 [4096, 512], replicated, may hold values from -0.09375 to 0.09375
- value_projection: bfloat16 [4096, 512], replicated, may hold values from -0.09375 to 0.09375
- key_norm_gain: float32 [128], replicated, may hold values from 0.1 to 1.9
- hidden: bfloat16 [16384, 4096], P(('ga', 'aa'), 'ba'), parts along dimension 0, may hold values from -6 to 6
- shared_query_base: bfloat16 [16384, 2048], P(('ga', 'aa'), 'ba'), parts along dimension 0, may hold values from -220 to 220
- adapter_down_matrix: bfloat16 [64, 4096, 16], P('aa'), may hold values from -0.09375 to 0.09375
- adapter_up_matrix: bfloat16 [64, 16, 2048], P('aa'), may hold values from -1.5 to 1.5
- tenant_adapter_index: int32 [16384, 1], P(('ga', 'aa')), parts along dimension 0, may hold values from 0 to 63; in each aligned block of 128 rows (0 to 127, 128 to 255, ...) at most 4 rows name the same one
- used_tile_count: int32 [16384], P(('ga', 'aa', 'ba')), parts along dimension 0, may hold values from 1 to 4
Outputs:
- attended: bfloat16 [16384, 2048], P(('ga', 'aa', 'ba')), parts along dimension 0
The draws below stay inside these ranges and needn't reach their ends.
There are 2 independent parts, one for each index of `ga`. The reference program is written for one: setup_inputs(seed, part) draws one part's arguments, and reference() takes and returns one part's arrays. A program takes and returns all parts, laid end to end along the dimension named above; an argument that names none is the same for every part. Nothing has to cross between parts.
Inputs may be any that keep to these rules, and one draw needn't show every extreme that they name: `tenant_adapter_index`: among the 128 requests of one index of aa (aligned blocks) no adapter is named more than 4 times.
All inputs are finite; a program needn't handle non-finite values.
Results may differ from the reference program's by a relative error of at most 0.012.
The reference program's roundings to bfloat16 on the way count: a program that leaves them out, or rounds other values in their place, can miss the bound.
Values may be sent and summed in bfloat16 or wider, within the bound.
A program may use at most 128 MiB of HBM per device.

```python
import math
import jax
import jax.numpy as jnp
import numpy as np
from jax import lax

MODEL_WIDTH = 4096
HEAD_WIDTH = 128
QUERY_HEADS = 16
KEY_VALUE_HEADS = 4
ADAPTER_RANK = 16
TILE_SLOTS = 4
TILE_TOKENS = 3
REQ_DEV = 128
REQUEST_TOTAL = 8192
ADAPTER_TOTAL = 64
MOST = 4
QUERY_WIDTH = 2048
KVW = 512


def draw_shared_query_base(key, part):
    key_values = jax.random.fold_in(jax.random.fold_in(key, 17), 0)
    normal_part = jnp.clip(jax.random.normal(key_values, (REQUEST_TOTAL, QUERY_WIDTH), jnp.float32), -6.0, 6.0)
    return normal_part.astype(jnp.bfloat16)


def place_ends(entries, own_key, smallest, largest):
    spot = [jax.random.randint(jax.random.fold_in(own_key, axis), (), 0, length) for axis, length in enumerate(entries.shape)]
    longest = entries.shape.index(max(entries.shape))
    next_to = spot[:longest] + [(spot[longest] + 1) % entries.shape[longest]] + spot[longest + 1:]
    return entries.at[tuple(spot)].set(smallest).at[tuple(next_to)].set(largest)


def level_of(own_key, extent, cuts, smallest, high):
    level = 1.0
    for dim, shards_of in cuts:
        steps = jax.random.uniform(jax.random.fold_in(jax.random.fold_in(own_key, 6), dim), (shards_of,), jnp.float32, smallest / len(cuts), high / len(cuts))
        level = level * jnp.repeat(jnp.exp(steps), extent[dim] // shards_of).reshape((-1,) + (1,) * (len(extent) - 1 - dim))
    return level


def assign_block(stream_key, own, number, rows, count, top, most, slope):
    order = jax.random.permutation(stream_key, count)
    heavy_load, common = shares(count, rows * top, most, slope, True), shares(count, rows * top, most, slope, False)
    places = jnp.arange(count)

    def named(sizes, offset_by):
        used = int((sizes > 0).sum())
        fixed = max(1, used // 4)
        passed = fixed + (places - fixed + offset_by * (used - fixed)) % max(1, count - fixed)
        return jnp.zeros((count,), jnp.int32).at[order[jnp.where(places < fixed, places, passed)]].set(jnp.asarray(sizes, jnp.int32))

    sizes = jnp.where(number % 4 == 0, named(heavy_load, number // 4), named(common, number - number // 4 - 1))
    mixed = jax.random.permutation(jax.random.fold_in(own, 3), count)
    donor, receiver = mixed[0:count // 2 * 2:2], mixed[1:count // 2 * 2:2]
    room = jnp.minimum(sizes[donor] - 1, most - sizes[receiver]) // 2
    room = jnp.where((donor == order[0]) | (receiver == order[0]) | (sizes[receiver] == 0), 0, jnp.maximum(room, 0))
    passed = jax.random.randint(jax.random.fold_in(own, 4), (count // 2,), 0, 1 << 20) % (room + 1)
    sizes = sizes.at[donor].add(-passed).at[receiver].add(passed)
    members = jnp.searchsorted(jnp.cumsum(sizes), jnp.arange(rows * top), side="right").astype(jnp.int32)
    table = members.reshape(top, rows).T
    table = table[jax.random.permutation(jax.random.fold_in(own, 1), rows)]
    offset_by = jax.random.randint(jax.random.fold_in(own, 2), (rows, 1), 0, top)
    return jnp.take_along_axis(table, (jnp.arange(top)[None, :] + offset_by) % top, axis=1)


def shares(amount, total, most, slope, full):
    weights = [(1 << 20) // math.isqrt(standing ** slope) + 1 for standing in range(1, amount + 1)]
    largest = most if full else min(most, max(-(-total // amount), total * weights[0] // sum(weights)))
    least = 1 if total - largest >= amount - 1 else 0
    holding, spare = [largest] + [least] * (amount - 1), total - largest - least * (amount - 1)
    while spare > 0:
        candidates = [i for i in range(1, amount) if holding[i] < largest] or [i for i in range(1, amount) if holding[i] < most]
        mass, remaining = sum([weights[i] for i in candidates]), spare
        for i in candidates:
            addition = min(most - holding[i], max(1, remaining * weights[i] // mass), spare)
            holding[i] = holding[i] + addition
            spare = spare - addition
    return np.array(holding)


def bell_draw(key, shape, spread, bound, pieces=(), kind=jnp.bfloat16):
    entries = spread * jax.random.normal(key, shape, jnp.float32)
    if pieces:
        entries = entries * level_of(key, shape, pieces, -0.22, 0.18)
    return jnp.clip(entries, -bound, bound).astype(kind)


def setup_inputs(seed: int = 0, part: int = 0) -> dict:
    keys = jax.random.split(jax.random.key(seed), 11)
    own_keys = jax.random.split(jax.random.fold_in(keys[10], part), 11)
    images = bell_draw(own_keys[0], (REQUEST_TOTAL, TILE_SLOTS * TILE_TOKENS, MODEL_WIDTH), 1.0, 6.0, ((0, 128),))
    key_projection = bell_draw(keys[1], (MODEL_WIDTH, KVW), MODEL_WIDTH ** -0.5, 0.09375)
    value_projection = bell_draw(keys[2], (MODEL_WIDTH, KVW), MODEL_WIDTH ** -0.5, 0.09375)
    key_norm_gain = jnp.clip(1.0 + 0.18 * jax.random.normal(keys[3], (HEAD_WIDTH,), jnp.float32), 0.1, 1.9)
    hidden = bell_draw(own_keys[4], (REQUEST_TOTAL, MODEL_WIDTH), 1.0, 6.0, ((0, 64), (1, 2)))
    shared_query_base = draw_shared_query_base(jax.random.fold_in(jax.random.fold_in(keys[10], part), 71), part)
    adapter_down_matrix = bell_draw(keys[6], (ADAPTER_TOTAL, MODEL_WIDTH, ADAPTER_RANK), MODEL_WIDTH ** -0.5, 0.09375, ((0, 64),))
    adapter_up_matrix = bell_draw(keys[7], (ADAPTER_TOTAL, ADAPTER_RANK, QUERY_WIDTH), ADAPTER_RANK ** -0.5, 1.5, ((0, 64),))
    tenant_adapter_index_keys = jax.random.split(jax.random.fold_in(own_keys[8], 1), REQUEST_TOTAL // REQ_DEV)
    tenant_adapter_index_turns = jax.random.permutation(jax.random.fold_in(own_keys[8], 3), REQUEST_TOTAL // REQ_DEV)
    tenant_adapter_index = jax.vmap(lambda own, number: assign_block(jax.random.fold_in(own_keys[8], 2), own, number, REQ_DEV, ADAPTER_TOTAL, 1, MOST, 2))(tenant_adapter_index_keys, tenant_adapter_index_turns).reshape((REQUEST_TOTAL, 1))
    used_tile_count = place_ends(jax.random.randint(own_keys[9], (REQUEST_TOTAL,), 1, TILE_SLOTS + 1), jax.random.fold_in(own_keys[9], 1), 1, TILE_SLOTS).astype(jnp.int32)
    return dict(images=images, key_projection=key_projection, value_projection=value_projection, key_norm_gain=key_norm_gain, hidden=hidden, shared_query_base=shared_query_base, adapter_down_matrix=adapter_down_matrix, adapter_up_matrix=adapter_up_matrix, tenant_adapter_index=tenant_adapter_index, used_tile_count=used_tile_count)


def reference(images, key_projection, value_projection, key_norm_gain, hidden, shared_query_base, adapter_down_matrix, adapter_up_matrix, tenant_adapter_index, used_tile_count):
    flattened_rows = images.reshape(REQUEST_TOTAL * TILE_SLOTS * TILE_TOKENS, MODEL_WIDTH)
    unnormed_keys = jnp.dot(flattened_rows, key_projection, preferred_element_type=jnp.float32).reshape(REQUEST_TOTAL, TILE_SLOTS * TILE_TOKENS, KEY_VALUE_HEADS, HEAD_WIDTH)
    key_scale = lax.rsqrt(lax.optimization_barrier(jnp.mean(unnormed_keys * unnormed_keys, axis=-1, keepdims=True)) + 1e-06)
    keys_all = (unnormed_keys * key_scale * key_norm_gain.astype(jnp.float32)).astype(jnp.bfloat16)
    gathered_values = jnp.dot(flattened_rows, value_projection, preferred_element_type=jnp.float32).astype(jnp.bfloat16)
    gathered_values = gathered_values.reshape(REQUEST_TOTAL, TILE_SLOTS * TILE_TOKENS, KEY_VALUE_HEADS, HEAD_WIDTH)
    owner_hot = (tenant_adapter_index[:, 0:1] == jnp.arange(ADAPTER_TOTAL, dtype=jnp.int32)[None, :]).astype(jnp.float32)
    widened_down_matrix = jnp.transpose(adapter_down_matrix, (1, 0, 2)).reshape(MODEL_WIDTH, ADAPTER_TOTAL * ADAPTER_RANK)
    low_all = jnp.dot(hidden, widened_down_matrix, preferred_element_type=jnp.float32).reshape(REQUEST_TOTAL, ADAPTER_TOTAL, ADAPTER_RANK)
    reduced_rank_part = lax.optimization_barrier(jnp.sum(low_all * owner_hot[:, :, None], axis=1))
    widened_reduced_part = owner_hot.astype(jnp.bfloat16)[:, :, None] * reduced_rank_part.astype(jnp.bfloat16)[:, None, :]
    adapter_query_delta = jnp.dot(widened_reduced_part.reshape(REQUEST_TOTAL, ADAPTER_TOTAL * ADAPTER_RANK), adapter_up_matrix.reshape(ADAPTER_TOTAL * ADAPTER_RANK, QUERY_WIDTH), preferred_element_type=jnp.float32).astype(jnp.bfloat16)
    query_rows = (shared_query_base.astype(jnp.float32) + adapter_query_delta.astype(jnp.float32)).astype(jnp.bfloat16)
    query_group_width = QUERY_HEADS // KEY_VALUE_HEADS
    query_four_axes = query_rows.reshape(REQUEST_TOTAL, KEY_VALUE_HEADS, query_group_width, HEAD_WIDTH).astype(jnp.float32)
    scores = jnp.einsum('rkgd,rjkd->rkgj', query_four_axes, keys_all.astype(jnp.float32)) / math.sqrt(HEAD_WIDTH)
    position = jnp.arange(TILE_SLOTS * TILE_TOKENS, dtype=jnp.int32) // TILE_TOKENS
    valid_rows = position[None, :] < used_tile_count[:, None]
    key_mask = valid_rows[:, None, None, :]
    scores = jnp.where(key_mask, scores, -jnp.inf)
    score_peak = lax.optimization_barrier(jnp.max(scores, axis=-1, keepdims=True))
    weights = jnp.exp(scores - score_peak)
    weight_total = lax.optimization_barrier(jnp.sum(weights, axis=-1))
    rounded = lax.optimization_barrier(weights.astype(jnp.bfloat16)).astype(jnp.float32)
    weighted = jnp.einsum('rkgj,rjkd->rkgd', rounded, gathered_values.astype(jnp.float32))
    attended = (weighted / weight_total[..., None]).reshape(REQUEST_TOTAL, QUERY_WIDTH).astype(jnp.bfloat16)
    return attended
```

```python
import functools
import math

import jax
import jax.numpy as jnp
from jax import lax
from jax.experimental import pallas as pl
from jax.experimental.pallas import tpu as pltpu
from jax.sharding import PartitionSpec as P

TILE_TOKENS = 3
BLOCK = 16
MESH = pl.DeviceIdType.MESH
F32 = jnp.float32
BF16 = jnp.bfloat16
NT = (((1,), (1,)), ((), ()))
TN = (((0,), (0,)), ((), ()))


def dot(a, b, dims=(((1,), (0,)), ((), ()))):
    return lax.dot_general(a, b, dims, preferred_element_type=F32)


def iota(shape, dim):
    return lax.broadcasted_iota(jnp.int32, shape, dim)


def kernel(
    side,
    most,
    images,
    wk,
    wv,
    gain,
    hidden,
    base,
    down,
    up,
    ids,
    used,
    out,
    images_v,
    wk_v,
    wv_v,
    gain_v,
    hidden_v,
    base_v,
    ids_v,
    used_v,
    adapters,
    packed,
    placing,
    received,
    low_own,
    low_other,
    raised,
    returned,
    q_own,
    q_send,
    q_other,
    keys,
    values,
    bias,
    local_sem,
    adapter_send,
    adapter_recv,
    row_send,
    row_recv,
    back_send,
    back_recv,
    low_send,
    low_recv,
    q_send_sem,
    q_recv_sem,
):
    me = lax.axis_index("aa")
    core = lax.axis_index("ba")
    y, x = me // side, me % side
    partner = {"ba": 1 - core}
    parity = (y + x) % 2
    banks = side * side
    group = side // 2
    chunk = group * most
    requests, half_model = hidden.shape
    half_query = base.shape[1]
    rank = up.shape[0]
    tokens, ours = keys.shape[0], keys.shape[1]
    head = gain.shape[1]

    def down_column(k):
        return {"aa": ((y + k) % side) * side + x}

    def along_row(k):
        return {"aa": y * side + (x + k) % side}

    own_slot = parity * (group + y // 2) + (1 - parity) * (x // 2)

    barrier = pltpu.get_barrier_semaphore()
    pl.semaphore_signal(barrier, inc=1, device_id=partner, device_id_type=MESH)
    for k in range(1, side):
        pl.semaphore_signal(barrier, inc=1, device_id=down_column(k), device_id_type=MESH)
        pl.semaphore_signal(barrier, inc=1, device_id=along_row(k), device_id_type=MESH)

    model_at = pl.multiple_of(core * half_model, half_model)
    query_at = pl.multiple_of(core * half_query, half_query)
    own_down = adapters.at[own_slot, :, pl.ds(0, half_model)]
    own_up = adapters.at[own_slot, :, pl.ds(half_model, half_query)]
    pairs = (
        (ids, ids_v),
        (hidden, hidden_v),
        (down.at[:, pl.ds(model_at, half_model)], own_down),
        (up.at[:, pl.ds(query_at, half_query)], own_up),
        (used, used_v),
        (gain, gain_v),
        (images, images_v),
        (wk, wk_v),
        (wv, wv_v),
        (base, base_v),
    )
    local = [pltpu.make_async_copy(s, d, local_sem.at[i]) for i, (s, d) in enumerate(pairs)]
    for copy in local:
        copy.start()

    local[0].wait()
    owner = ids_v[...]
    hot = (iota((banks, requests), 0) == owner).astype(BF16)
    earlier = (iota((requests, requests), 0) < iota((requests, requests), 1)).astype(BF16)
    before = dot(hot, earlier)
    standing = jnp.sum(before * hot.astype(F32), axis=0, keepdims=True).astype(jnp.int32)
    shift = side.bit_length() - 1
    owner_y, owner_x = owner >> shift, owner & (side - 1)
    odd = (owner_y + owner_x) & 1
    place = jnp.where(
        odd == 0,
        owner_y * group + (owner_x >> 1),
        banks // 2 + owner_x * group + (owner_y >> 1),
    )
    slot = place * most + standing
    placing[...] = (iota((banks * most, requests), 0) == slot).astype(BF16)
    local[1].wait()
    packed[...] = (
        dot(placing[...], hidden_v[...]).astype(BF16).reshape(2 * side, chunk, half_model)
    )
    received[y] = packed[y]
    received[side + x] = packed[side + x]
    local[2].wait()
    local[3].wait()

    pl.semaphore_wait(barrier, 2 * side - 1)

    sends = []

    def send(source, target, send_sem, recv_sem, device):
        copy = pltpu.make_async_remote_copy(
            src_ref=source,
            dst_ref=target,
            send_sem=send_sem,
            recv_sem=recv_sem,
            device_id=device,
            device_id_type=MESH,
        )
        copy.start()
        sends.append(copy)
        return copy

    order = sorted(range(1, side), key=lambda k: -min(k, side - k))
    for k in order:
        peer = parity * ((y + k) % side * side + x) + (1 - parity) * (y * side + (x + k) % side)
        send(
            adapters.at[own_slot],
            adapters.at[own_slot],
            adapter_send.at[k],
            adapter_recv.at[own_slot],
            {"aa": peer},
        )
    for k in order:
        to_y, to_x = (y + k) % side, (x + k) % side
        send(packed.at[to_y], received.at[y], row_send.at[k], row_recv.at[y], down_column(k))
        send(
            packed.at[side + to_x],
            received.at[side + x],
            row_send.at[side + k],
            row_recv.at[side + x],
            along_row(k),
        )

    local[4].wait()
    local[5].wait()
    local[6].wait()
    local[7].wait()
    wide = 2 * head

    def project_keys(n, carry):
        at = pl.multiple_of(n * wide, wide)
        raw = dot(images_v[...], wk_v[:, pl.ds(at, wide)])
        for part in range(2):
            one = raw[:, part * head : (part + 1) * head]
            scale = lax.rsqrt(jnp.mean(one * one, axis=1, keepdims=True) + 1e-06)
            keys[:, :, pl.ds(pl.multiple_of(at + part * head, head), head)] = (
                (one * scale * gain_v[...]).astype(BF16).reshape(tokens, ours, head)
            )
        return carry

    lax.fori_loop(0, wk.shape[1] // wide, project_keys, 0)
    local[8].wait()

    def project_values(n, carry):
        at = pl.multiple_of(n * wide, wide)
        raw = dot(images_v[...], wv_v[:, pl.ds(at, wide)])
        values[:, :, pl.ds(at, wide)] = raw.astype(BF16).reshape(tokens, ours, wide)
        return carry

    lax.fori_loop(0, wv.shape[1] // wide, project_values, 0)

    lanes = tokens * BLOCK
    heads_each = (2 * half_query // head) // (wk.shape[1] // head)
    rows = heads_each * BLOCK
    token = iota((1, lanes), 1) // BLOCK
    tile = jnp.zeros((1, lanes), jnp.int32)
    for edge in range(TILE_TOKENS, tokens, TILE_TOKENS):
        tile = tile + (token >= edge).astype(jnp.int32)
    counts = jnp.broadcast_to(used_v[...].astype(F32), (8, ours)).astype(BF16)
    same = (iota((rows, lanes), 0) & (BLOCK - 1)) == (iota((rows, lanes), 1) & (BLOCK - 1))
    for b in range(ours // BLOCK):
        spread = (
            iota((ours, lanes), 0) == b * BLOCK + (iota((ours, lanes), 1) & (BLOCK - 1))
        ).astype(BF16)
        count = dot(counts, spread)[0:1]
        bias[b] = jnp.where(same & (tile.astype(F32) < count), 0.0, -1e30)

    def arrived(ref, send_sem, recv_sem):
        pltpu.make_async_remote_copy(
            src_ref=ref,
            dst_ref=ref,
            send_sem=send_sem,
            recv_sem=recv_sem,
            device_id=partner,
            device_id_type=MESH,
        ).wait_recv()

    for k in range(1, side):
        other = (own_slot + k) % side
        arrived(adapters.at[other], adapter_send.at[k], adapter_recv.at[other])
    slots = side * chunk
    in_slot = (iota((slots, group * rank), 0) & (chunk - 1)) // most
    keep = in_slot == iota((slots, group * rank), 1) // rank
    for kind, here in ((0, y), (1, x)):
        for k in range(1, side):
            source = kind * side + (here + k) % side
            arrived(received.at[source], row_send.at[k], row_recv.at[source])
        low = dot(
            received[kind * side : (kind + 1) * side].reshape(slots, half_model),
            adapters[kind * group : (kind + 1) * group, :, :half_model].reshape(
                group * rank, half_model
            ),
            NT,
        )
        low_own[kind] = jnp.where(keep, low, 0.0)
    send(low_own, low_other, low_send, low_recv, partner)
    arrived(low_other, low_send, low_recv)
    for kind in range(2):
        low = (low_own[kind] + low_other[kind]).astype(BF16)
        result = dot(
            low,
            adapters[kind * group : (kind + 1) * group, :, half_model:].reshape(
                group * rank, half_query
            ),
        )
        raised[kind * side : (kind + 1) * side] = result.astype(BF16).reshape(
            side, chunk, half_query
        )
    returned[y] = raised[y]
    returned[side + x] = raised[side + x]
    for k in order:
        to_y, to_x = (y + k) % side, (x + k) % side
        send(raised.at[to_y], returned.at[y], back_send.at[k], back_recv.at[y], down_column(k))
        send(
            raised.at[side + to_x],
            returned.at[side + x],
            back_send.at[side + k],
            back_recv.at[side + x],
            along_row(k),
        )
    local[9].wait()
    for kind, here in ((0, y), (1, x)):
        for k in range(1, side):
            source = kind * side + (here + k) % side
            arrived(returned.at[source], back_send.at[k], back_recv.at[source])
    delta = dot(placing[...], returned[...].reshape(banks * most, half_query), TN)
    query = (base_v[...].astype(F32) + delta).astype(BF16)
    q_own[...] = query.reshape(2, ours, half_query)
    q_send[...] = q_own[1 - core]
    send(q_send, q_other, q_send_sem, q_recv_sem, partner)

    def attend(q, part):
        for b in range(ours // BLOCK):
            at = slice(b * BLOCK, (b + 1) * BLOCK)
            for g in range(half_query // head // heads_each):
                first = part * half_query + g * heads_each * head
                kv = pl.multiple_of(
                    part * (half_query // heads_each) + g * head, head
                )
                block = jnp.concatenate(
                    [
                        q[at, (g * heads_each + i) * head : (g * heads_each + i + 1) * head]
                        for i in range(heads_each)
                    ],
                    axis=0,
                )
                key = keys[:, at, pl.ds(kv, head)].reshape(lanes, head)
                value = values[:, at, pl.ds(kv, head)].reshape(lanes, head)
                score = dot(block, key, NT) * (1.0 / math.sqrt(head)) + bias[b]
                weight = jnp.exp(score - jnp.max(score, axis=1, keepdims=True))
                total = jnp.sum(weight, axis=1, keepdims=True)
                result = (dot(weight.astype(BF16), value) / total).astype(BF16)
                for i in range(heads_each):
                    out[at, pl.ds(pl.multiple_of(first + i * head, head), head)] = result[
                        i * BLOCK : (i + 1) * BLOCK
                    ]

    attend(q_own[core], core)
    arrived(q_other, q_send_sem, q_recv_sem)
    attend(q_other[...], 1 - core)
    for copy in sends:
        copy.wait_send()


def on_device(
    side,
    images,
    key_projection,
    value_projection,
    key_norm_gain,
    hidden,
    shared_query_base,
    adapter_down_matrix,
    adapter_up_matrix,
    tenant_adapter_index,
    used_tile_count,
):
    ours, tokens, model = images.shape
    requests, half_model = hidden.shape
    half_query = shared_query_base.shape[1]
    head = key_norm_gain.shape[0]
    kvw = key_projection.shape[1]
    banks = side * side
    most = 2 * requests // banks
    group = side // 2
    chunk = group * most
    rank = adapter_up_matrix.shape[1]
    heads_each = 2 * half_query // kvw
    args = (
        jnp.transpose(images, (1, 0, 2)).reshape(tokens * ours, model),
        key_projection,
        value_projection,
        key_norm_gain.reshape(1, head),
        hidden,
        shared_query_base,
        jnp.transpose(adapter_down_matrix[0]),
        adapter_up_matrix[0],
        tenant_adapter_index.reshape(1, requests),
        used_tile_count.reshape(1, ours),
    )
    dma = pltpu.SemaphoreType.DMA
    return pl.pallas_call(
        functools.partial(kernel, side, most),
        out_shape=jax.ShapeDtypeStruct((ours, 2 * half_query), BF16),
        in_specs=[pl.BlockSpec(memory_space=pl.ANY)] * len(args),
        out_specs=pl.BlockSpec(memory_space=pltpu.VMEM),
        scratch_shapes=[
            pltpu.VMEM((tokens * ours, model), BF16),
            pltpu.VMEM((model, kvw), BF16),
            pltpu.VMEM((model, kvw), BF16),
            pltpu.VMEM((1, head), F32),
            pltpu.VMEM((requests, half_model), BF16),
            pltpu.VMEM((requests, half_query), BF16),
            pltpu.VMEM((1, requests), jnp.int32),
            pltpu.VMEM((1, ours), jnp.int32),
            pltpu.VMEM((side, rank, half_model + half_query), BF16),
            pltpu.VMEM((2 * side, chunk, half_model), BF16),
            pltpu.VMEM((banks * most, requests), BF16),
            pltpu.VMEM((2 * side, chunk, half_model), BF16),
            pltpu.VMEM((2, side * chunk, group * rank), F32),
            pltpu.VMEM((2, side * chunk, group * rank), F32),
            pltpu.VMEM((2 * side, chunk, half_query), BF16),
            pltpu.VMEM((2 * side, chunk, half_query), BF16),
            pltpu.VMEM((2, ours, half_query), BF16),
            pltpu.VMEM((ours, half_query), BF16),
            pltpu.VMEM((ours, half_query), BF16),
            pltpu.VMEM((tokens, ours, kvw), BF16),
            pltpu.VMEM((tokens, ours, kvw), BF16),
            pltpu.VMEM((ours // BLOCK, heads_each * BLOCK, tokens * BLOCK), F32),
            dma((10,)),
            dma((side,)),
            dma((side,)),
            dma((2 * side,)),
            dma((2 * side,)),
            dma((2 * side,)),
            dma((2 * side,)),
            dma(()),
            dma(()),
            dma(()),
            dma(()),
        ],
        compiler_params=pltpu.CompilerParams(collective_id=0, has_side_effects=True),
        name="adapter_attention",
    )(*args)


def solution(mesh):
    placed = (
        P(("ga", "aa", "ba"), None, None),
        P(),
        P(),
        P(),
        P(("ga", "aa"), "ba"),
        P(("ga", "aa"), "ba"),
        P("aa", None, None),
        P("aa", None, None),
        P(("ga", "aa"), None),
        P(("ga", "aa", "ba")),
    )
    return jax.shard_map(
        functools.partial(on_device, math.isqrt(mesh.shape["aa"])),
        mesh=mesh,
        in_specs=placed,
        out_specs=P(("ga", "aa", "ba"), None),
        check_vma=False,
    )
```

```python
import functools
import math

import jax
import jax.numpy as jnp
from jax import lax
from jax.experimental import pallas as pl
from jax.experimental.pallas import tpu as pltpu
from jax.sharding import PartitionSpec as P

TILE_TOKENS = 3
BLOCK = 16
MESH = pl.DeviceIdType.MESH
F32 = jnp.float32
BF16 = jnp.bfloat16
NT = (((1,), (1,)), ((), ()))
TN = (((0,), (0,)), ((), ()))


def dot(a, b, dims=(((1,), (0,)), ((), ()))):
    return lax.dot_general(a, b, dims, preferred_element_type=F32)


def iota(shape, dim):
    return lax.broadcasted_iota(jnp.int32, shape, dim)


def kernel(
    side,
    most,
    images,
    wk,
    wv,
    gain,
    hidden,
    base,
    down,
    up,
    ids,
    used,
    out,
    images_v,
    wk_v,
    wv_v,
    gain_v,
    hidden_v,
    base_v,
    ids_v,
    used_v,
    adapters,
    packed,
    placing,
    received,
    low_own,
    low_other,
    raised,
    returned,
    q_own,
    q_send,
    q_other,
    keys,
    values,
    bias,
    scores,
    weights,
    totals,
    local_sem,
    adapter_send,
    adapter_recv,
    row_send,
    row_recv,
    back_send,
    back_recv,
    low_send,
    low_recv,
    q_send_sem,
    q_recv_sem,
):
    me = lax.axis_index("aa")
    core = lax.axis_index("ba")
    y, x = me // side, me % side
    partner = {"ba": 1 - core}
    parity = (y + x) % 2
    banks = side * side
    group = side // 2
    chunk = group * most
    requests, half_model = hidden.shape
    half_query = base.shape[1]
    rank = up.shape[0]
    tokens, ours = keys.shape[0], keys.shape[1]
    head = gain.shape[1]

    def down_column(k):
        return {"aa": ((y + k) % side) * side + x}

    def along_row(k):
        return {"aa": y * side + (x + k) % side}

    def neighbour(ring, k):
        across = y * side + (x + k + side) % side
        along = (y + k + side) % side * side + x
        row_wise = 1 - parity if ring == 1 else parity
        return {"aa": row_wise * across + (1 - row_wise) * along}

    def slot_of(ring, k):
        even = (x + k + side) % side // 2
        odd = group + (y + k + side) % side // 2
        row_wise = 1 - parity if ring == 1 else parity
        return row_wise * even + (1 - row_wise) * odd

    own_slot = slot_of(1, 0)

    barrier = pltpu.get_barrier_semaphore()
    pl.semaphore_signal(barrier, inc=1, device_id=partner, device_id_type=MESH)
    for k in range(1, side):
        pl.semaphore_signal(barrier, inc=1, device_id=down_column(k), device_id_type=MESH)
        pl.semaphore_signal(barrier, inc=1, device_id=along_row(k), device_id_type=MESH)

    model_at = pl.multiple_of(core * half_model, half_model)
    query_at = pl.multiple_of(core * half_query, half_query)
    own_down = adapters.at[own_slot, :, pl.ds(0, half_model)]
    own_up = adapters.at[own_slot, :, pl.ds(half_model, half_query)]
    pairs = (
        (down.at[:, pl.ds(model_at, half_model)], own_down),
        (up.at[:, pl.ds(query_at, half_query)], own_up),
        (ids, ids_v),
        (hidden, hidden_v),
        (images, images_v),
        (wk, wk_v),
        (wv, wv_v),
        (gain, gain_v),
        (used, used_v),
        (base, base_v),
    )
    local = [pltpu.make_async_copy(s, d, local_sem.at[i]) for i, (s, d) in enumerate(pairs)]
    for copy in local[:4]:
        copy.start()

    sends = []

    def send(source, target, send_sem, recv_sem, device):
        copy = pltpu.make_async_remote_copy(
            src_ref=source,
            dst_ref=target,
            send_sem=send_sem,
            recv_sem=recv_sem,
            device_id=device,
            device_id_type=MESH,
        )
        copy.start()
        sends.append(copy)

    def arrived(ref, send_sem, recv_sem):
        pltpu.make_async_remote_copy(
            src_ref=ref,
            dst_ref=ref,
            send_sem=send_sem,
            recv_sem=recv_sem,
            device_id=partner,
            device_id_type=MESH,
        ).wait_recv()

    last = side // 2
    turn = 1 - 2 * core

    def ways(step):
        return (1, -1) if step < last else (turn,)

    def pass_on(step):
        ring = 1 if step % 2 else 2
        for way in ways(step):
            at = slot_of(ring, -way * (step - 1))
            send(
                adapters.at[at],
                adapters.at[at],
                adapter_send.at[passes.pop()],
                adapter_recv.at[at],
                neighbour(ring, way),
            )

    def taken(step):
        ring = 2 if step % 2 else 1
        for way in ways(step):
            at = slot_of(ring, -way * step)
            arrived(adapters.at[at], adapter_send.at[0], adapter_recv.at[at])

    passes = list(range(side))

    def send_rows(distance):
        for k in (distance, side - distance) if distance < last else (distance,):
            to_y, to_x = (y + k) % side, (x + k) % side
            send(packed.at[to_y], received.at[y], row_send.at[k], row_recv.at[y], down_column(k))
            send(
                packed.at[side + to_x],
                received.at[side + x],
                row_send.at[side + k],
                row_recv.at[side + x],
                along_row(k),
            )

    local[0].wait()
    local[1].wait()
    pl.semaphore_wait(barrier, 2 * side - 1)
    pass_on(1)

    local[2].wait()
    owner = ids_v[...]
    hot = (iota((banks, requests), 0) == owner).astype(BF16)
    earlier = (iota((requests, requests), 0) < iota((requests, requests), 1)).astype(BF16)
    before = dot(hot, earlier)
    standing = jnp.sum(before * hot.astype(F32), axis=0, keepdims=True).astype(jnp.int32)
    shift = side.bit_length() - 1
    owner_y, owner_x = owner >> shift, owner & (side - 1)
    odd = (owner_y + owner_x) & 1
    place = jnp.where(
        odd == 0,
        owner_y * group + (owner_x >> 1),
        banks // 2 + owner_x * group + (owner_y >> 1),
    )
    slot = place * most + standing
    placing[...] = (iota((banks * most, requests), 0) == slot).astype(BF16)
    local[3].wait()
    for copy in local[4:]:
        copy.start()
    packed[...] = (
        dot(placing[...], hidden_v[...]).astype(BF16).reshape(2 * side, chunk, half_model)
    )
    received[y] = packed[y]
    received[side + x] = packed[side + x]
    distances = sorted(range(1, last + 1), key=lambda d: -min(d, side - d) * (1 if d < last else 0.6))
    send_rows(distances[0])

    local[4].wait()
    local[5].wait()
    local[7].wait()
    wide = 2 * head
    key_parts = wk.shape[1] // wide

    def project_keys(n):
        at = n * wide
        raw = dot(images_v[...], wk_v[:, at : at + wide])
        for part in range(2):
            one = raw[:, part * head : (part + 1) * head]
            scale = lax.rsqrt(jnp.mean(one * one, axis=1, keepdims=True) + 1e-06)
            keys[:, :, at + part * head : at + (part + 1) * head] = (
                (one * scale * gain_v[...]).astype(BF16).reshape(tokens, ours, head)
            )

    def project_values(n):
        at = n * wide
        raw = dot(images_v[...], wv_v[:, at : at + wide])
        values[:, :, at : at + wide] = raw.astype(BF16).reshape(tokens, ours, wide)

    for part in range(2 * key_parts):
        if part == key_parts:
            local[6].wait()
        if part < key_parts:
            project_keys(part)
        else:
            project_values(part - key_parts)
        if part + 1 < last:
            taken(part + 1)
            pass_on(part + 2)
            send_rows(distances[part + 1])
    for step in range(2 * key_parts + 1, last):
        taken(step)
        pass_on(step + 1)
        send_rows(distances[step])
    local[8].wait()

    lanes = tokens * BLOCK
    heads_each = (2 * half_query // head) // (wk.shape[1] // head)
    rows = heads_each * BLOCK
    token = iota((1, lanes), 1) // BLOCK
    tile = jnp.zeros((1, lanes), jnp.int32)
    for edge in range(TILE_TOKENS, tokens, TILE_TOKENS):
        tile = tile + (token >= edge).astype(jnp.int32)
    counts = jnp.broadcast_to(used_v[...].astype(F32), (8, ours)).astype(BF16)
    same = (iota((rows, lanes), 0) & (BLOCK - 1)) == (iota((rows, lanes), 1) & (BLOCK - 1))
    for b in range(ours // BLOCK):
        spread = (
            iota((ours, lanes), 0) == b * BLOCK + (iota((ours, lanes), 1) & (BLOCK - 1))
        ).astype(BF16)
        count = dot(counts, spread)[0:1]
        bias[b] = jnp.where(same & (tile.astype(F32) < count), 0.0, -1e30)

    taken(last)
    slots = side * chunk
    in_slot = (iota((slots, group * rank), 0) & (chunk - 1)) // most
    keep = in_slot == iota((slots, group * rank), 1) // rank
    for kind, here in ((0, y), (1, x)):
        for k in range(1, side):
            source = kind * side + (here + k) % side
            arrived(received.at[source], row_send.at[k], row_recv.at[source])
        low = dot(
            received[kind * side : (kind + 1) * side].reshape(slots, half_model),
            adapters[kind * group : (kind + 1) * group, :, :half_model].reshape(
                group * rank, half_model
            ),
            NT,
        )
        low_own[kind] = jnp.where(keep, low, 0.0)
        send(
            low_own.at[kind], low_other.at[kind], low_send.at[kind], low_recv.at[kind], partner
        )
    for kind, here in ((0, y), (1, x)):
        arrived(low_other.at[kind], low_send.at[kind], low_recv.at[kind])
        low = (low_own[kind] + low_other[kind]).astype(BF16)
        result = dot(
            low,
            adapters[kind * group : (kind + 1) * group, :, half_model:].reshape(
                group * rank, half_query
            ),
        )
        raised[kind * side : (kind + 1) * side] = result.astype(BF16).reshape(
            side, chunk, half_query
        )
        returned[kind * side + here] = raised[kind * side + here]
        for distance in range(last, 0, -1):
            for k in (distance, side - distance) if distance < last else (distance,):
                send(
                    raised.at[kind * side + (here + k) % side],
                    returned.at[kind * side + here],
                    back_send.at[kind * side + k],
                    back_recv.at[kind * side + here],
                    along_row(k) if kind else down_column(k),
                )
    local[9].wait()
    for kind, here in ((0, y), (1, x)):
        for k in range(1, side):
            source = kind * side + (here + k) % side
            arrived(returned.at[source], back_send.at[k], back_recv.at[source])
    delta = dot(placing[...], returned[...].reshape(banks * most, half_query), TN)
    query = (base_v[...].astype(F32) + delta).astype(BF16)
    q_own[...] = query.reshape(2, ours, half_query)
    q_send[...] = q_own[1 - core]
    send(q_send, q_other, q_send_sem, q_recv_sem, partner)

    heads_kv = half_query // head // heads_each
    cells = [(b, g) for b in range(ours // BLOCK) for g in range(heads_kv)]

    def attend(q, part):
        first_kv = part * (heads_kv * head)
        for n, (b, g) in enumerate(cells):
            at = slice(b * BLOCK, (b + 1) * BLOCK)
            block = jnp.concatenate(
                [
                    q[at, (g * heads_each + i) * head : (g * heads_each + i + 1) * head]
                    for i in range(heads_each)
                ],
                axis=0,
            )
            key = keys[:, at, pl.ds(pl.multiple_of(first_kv + g * head, head), head)]
            scores[n] = (
                dot(block, key.reshape(lanes, head), NT) * (1.0 / math.sqrt(head)) + bias[b]
            )
        peaks = jnp.max(scores[...], axis=2, keepdims=True)
        weight = jnp.exp(scores[...] - peaks)
        totals[...] = jnp.broadcast_to(
            jnp.sum(weight, axis=2, keepdims=True), totals.shape
        )
        weights[...] = weight.astype(BF16)
        for n, (b, g) in enumerate(cells):
            at = slice(b * BLOCK, (b + 1) * BLOCK)
            value = values[:, at, pl.ds(pl.multiple_of(first_kv + g * head, head), head)]
            result = (dot(weights[n], value.reshape(lanes, head)) / totals[n]).astype(BF16)
            for i in range(heads_each):
                column = part * half_query + (g * heads_each + i) * head
                out[at, pl.ds(pl.multiple_of(column, head), head)] = result[
                    i * BLOCK : (i + 1) * BLOCK
                ]

    attend(q_own[core], core)
    arrived(q_other, q_send_sem, q_recv_sem)
    attend(q_other[...], 1 - core)
    for copy in sends:
        copy.wait_send()


def on_device(
    side,
    images,
    key_projection,
    value_projection,
    key_norm_gain,
    hidden,
    shared_query_base,
    adapter_down_matrix,
    adapter_up_matrix,
    tenant_adapter_index,
    used_tile_count,
):
    ours, tokens, model = images.shape
    requests, half_model = hidden.shape
    half_query = shared_query_base.shape[1]
    head = key_norm_gain.shape[0]
    kvw = key_projection.shape[1]
    banks = side * side
    most = 2 * requests // banks
    group = side // 2
    chunk = group * most
    rank = adapter_up_matrix.shape[1]
    heads_each = 2 * half_query // kvw
    cells = ours // BLOCK * (half_query // head // heads_each)
    args = (
        jnp.transpose(images, (1, 0, 2)).reshape(tokens * ours, model),
        key_projection,
        value_projection,
        key_norm_gain.reshape(1, head),
        hidden,
        shared_query_base,
        jnp.transpose(adapter_down_matrix[0]),
        adapter_up_matrix[0],
        tenant_adapter_index.reshape(1, requests),
        used_tile_count.reshape(1, ours),
    )
    dma = pltpu.SemaphoreType.DMA
    return pl.pallas_call(
        functools.partial(kernel, side, most),
        out_shape=jax.ShapeDtypeStruct((ours, 2 * half_query), BF16),
        in_specs=[pl.BlockSpec(memory_space=pl.ANY)] * len(args),
        out_specs=pl.BlockSpec(memory_space=pltpu.VMEM),
        scratch_shapes=[
            pltpu.VMEM((tokens * ours, model), BF16),
            pltpu.VMEM((model, kvw), BF16),
            pltpu.VMEM((model, kvw), BF16),
            pltpu.VMEM((1, head), F32),
            pltpu.VMEM((requests, half_model), BF16),
            pltpu.VMEM((requests, half_query), BF16),
            pltpu.VMEM((1, requests), jnp.int32),
            pltpu.VMEM((1, ours), jnp.int32),
            pltpu.VMEM((side, rank, half_model + half_query), BF16),
            pltpu.VMEM((2 * side, chunk, half_model), BF16),
            pltpu.VMEM((banks * most, requests), BF16),
            pltpu.VMEM((2 * side, chunk, half_model), BF16),
            pltpu.VMEM((2, side * chunk, group * rank), F32),
            pltpu.VMEM((2, side * chunk, group * rank), F32),
            pltpu.VMEM((2 * side, chunk, half_query), BF16),
            pltpu.VMEM((2 * side, chunk, half_query), BF16),
            pltpu.VMEM((2, ours, half_query), BF16),
            pltpu.VMEM((ours, half_query), BF16),
            pltpu.VMEM((ours, half_query), BF16),
            pltpu.VMEM((tokens, ours, kvw), BF16),
            pltpu.VMEM((tokens, ours, kvw), BF16),
            pltpu.VMEM((ours // BLOCK, heads_each * BLOCK, tokens * BLOCK), F32),
            pltpu.VMEM((cells, heads_each * BLOCK, tokens * BLOCK), F32),
            pltpu.VMEM((cells, heads_each * BLOCK, tokens * BLOCK), BF16),
            pltpu.VMEM((cells, heads_each * BLOCK, head), F32),
            dma((10,)),
            dma((side,)),
            dma((side,)),
            dma((2 * side,)),
            dma((2 * side,)),
            dma((2 * side,)),
            dma((2 * side,)),
            dma((2,)),
            dma((2,)),
            dma(()),
            dma(()),
        ],
        compiler_params=pltpu.CompilerParams(collective_id=0, has_side_effects=True),
        name="adapter_attention",
    )(*args)


def solution(mesh):
    placed = (
        P(("ga", "aa", "ba"), None, None),
        P(),
        P(),
        P(),
        P(("ga", "aa"), "ba"),
        P(("ga", "aa"), "ba"),
        P("aa", None, None),
        P("aa", None, None),
        P(("ga", "aa"), None),
        P(("ga", "aa", "ba")),
    )
    return jax.shard_map(
        functools.partial(on_device, math.isqrt(mesh.shape["aa"])),
        mesh=mesh,
        in_specs=placed,
        out_specs=P(("ga", "aa", "ba"), None),
        check_vma=False,
    )
```

```python
import functools
import math

import jax
import jax.numpy as jnp
from jax import lax
from jax.experimental import pallas as pl
from jax.experimental.pallas import tpu as pltpu
from jax.sharding import PartitionSpec as P

TILE_TOKENS = 3
BLOCK = 16
MESH = pl.DeviceIdType.MESH
F32 = jnp.float32
BF16 = jnp.bfloat16
NT = (((1,), (1,)), ((), ()))
TN = (((0,), (0,)), ((), ()))


def dot(a, b, dims=(((1,), (0,)), ((), ()))):
    return lax.dot_general(a, b, dims, preferred_element_type=F32)


def iota(shape, dim):
    return lax.broadcasted_iota(jnp.int32, shape, dim)


def kernel(
    side,
    most,
    images,
    wk,
    wv,
    gain,
    hidden,
    base,
    down,
    up,
    ids,
    used,
    out,
    images_v,
    wk_v,
    wv_v,
    gain_v,
    hidden_v,
    base_v,
    ids_v,
    used_v,
    adapters,
    packed,
    placing,
    received,
    low_own,
    low_other,
    raised,
    returned,
    q_own,
    q_send,
    q_other,
    keys,
    values,
    bias,
    scores,
    weights,
    totals,
    gate,
    local_sem,
    adapter_send,
    adapter_recv,
    row_send,
    row_recv,
    back_send,
    back_recv,
    low_send,
    low_recv,
    q_send_sem,
    q_recv_sem,
):
    me = lax.axis_index("aa")
    core = lax.axis_index("ba")
    y, x = me // side, me % side
    partner = {"ba": 1 - core}
    parity = (y + x) % 2
    banks = side * side
    group = side // 2
    chunk = group * most
    requests, half_model = hidden.shape
    half_query = base.shape[1]
    rank = up.shape[0]
    tokens, ours = keys.shape[0], keys.shape[1]
    head = gain.shape[1]

    own_slot = (1 - parity) * (x // 2) + parity * (group + y // 2)

    def rank_of(index):
        return (index + banks - 1 + core) % banks

    mine = rank_of(me)
    last_column = jnp.where((core == 0) & (x == 0), 1, 0)
    last_row = jnp.where((core == 0) & (y == 0), 1, 0)
    around = [
        (index, gate_at, own_gate)
        for k in range(1, side)
        for index, gate_at, own_gate in (
            ((y + k) % side * side + x, (y + k) % side, y),
            (y * side + (x + k) % side, side + (x + k) % side, side + x),
        )
    ]

    barrier = pltpu.get_barrier_semaphore()
    pl.semaphore_signal(barrier, inc=1, device_id={"aa": me}, device_id_type=MESH)
    earlier_peers = 2 - core
    for index, gate_at, own_gate in around:
        earlier_peers = earlier_peers + jnp.where(rank_of(index) < mine, 1, 0)

        @pl.when(rank_of(index) > mine)
        def _(index=index):
            pl.semaphore_signal(barrier, inc=1, device_id={"aa": index}, device_id_type=MESH)

    @pl.when(core == 1)
    def _():
        pl.semaphore_signal(barrier, inc=1, device_id=partner, device_id_type=MESH)

    model_at = pl.multiple_of(core * half_model, half_model)
    query_at = pl.multiple_of(core * half_query, half_query)
    own_down = adapters.at[own_slot, :, pl.ds(0, half_model)]
    own_up = adapters.at[own_slot, :, pl.ds(half_model, half_query)]
    pairs = (
        (down.at[:, pl.ds(model_at, half_model)], own_down),
        (up.at[:, pl.ds(query_at, half_query)], own_up),
        (ids, ids_v),
        (hidden, hidden_v),
        (images, images_v),
        (wk, wk_v),
        (wv, wv_v),
        (gain, gain_v),
        (used, used_v),
        (base, base_v),
    )
    local = [pltpu.make_async_copy(s, d, local_sem.at[i]) for i, (s, d) in enumerate(pairs)]
    for copy in local[:4]:
        copy.start()

    def start(source, target, send_sem, recv_sem, device):
        pltpu.make_async_remote_copy(
            src_ref=source,
            dst_ref=target,
            send_sem=send_sem,
            recv_sem=recv_sem,
            device_id=device,
            device_id_type=MESH,
        ).start()

    def left(ref, send_sem, recv_sem):
        pltpu.make_async_remote_copy(
            src_ref=ref,
            dst_ref=ref,
            send_sem=send_sem,
            recv_sem=recv_sem,
            device_id=partner,
            device_id_type=MESH,
        ).wait_send()

    def arrived(ref, send_sem, recv_sem):
        pltpu.make_async_remote_copy(
            src_ref=ref,
            dst_ref=ref,
            send_sem=send_sem,
            recv_sem=recv_sem,
            device_id=partner,
            device_id_type=MESH,
        ).wait_recv()

    def to_row(p, adapter, rows):
        at = (p + last_row) % side
        index = y * side + at

        @pl.when(at != x)
        def _():
            if adapter:

                @pl.when(rank_of(index) > mine)
                def _():
                    pl.semaphore_wait(gate.at[side + at], 1)

                @pl.when(parity == 0)
                def _():
                    start(
                        adapters.at[own_slot],
                        adapters.at[own_slot],
                        adapter_send.at[at],
                        adapter_recv.at[own_slot],
                        {"aa": index},
                    )

            if rows:
                start(
                    packed.at[side + at],
                    received.at[side + x],
                    row_send.at[side + at],
                    row_recv.at[side + x],
                    {"aa": index},
                )

    def to_column(p):
        at = (p + last_column) % side
        index = at * side + x

        @pl.when(at != y)
        def _():
            @pl.when(rank_of(index) > mine)
            def _():
                pl.semaphore_wait(gate.at[at], 1)

            @pl.when(parity == 1)
            def _():
                start(
                    adapters.at[own_slot],
                    adapters.at[own_slot],
                    adapter_send.at[at],
                    adapter_recv.at[own_slot],
                    {"aa": index},
                )

            start(
                packed.at[at],
                received.at[y],
                row_send.at[at],
                row_recv.at[y],
                {"aa": index},
            )

    pl.semaphore_wait(barrier, earlier_peers)
    for index, gate_at, own_gate in around:

        @pl.when(rank_of(index) < mine)
        def _(index=index, own_gate=own_gate):
            pl.semaphore_signal(
                gate.at[own_gate], inc=1, device_id={"aa": index}, device_id_type=MESH
            )

    @pl.when(core == 0)
    def _():
        pl.semaphore_signal(gate.at[2 * side], inc=1, device_id=partner, device_id_type=MESH)

    local[0].wait()
    local[1].wait()
    for p in range(side - 1):
        to_row(p, True, False)

    local[2].wait()
    owner = ids_v[...]
    hot = (iota((banks, requests), 0) == owner).astype(BF16)
    earlier = (iota((requests, requests), 0) < iota((requests, requests), 1)).astype(BF16)
    before = dot(hot, earlier)
    standing = jnp.sum(before * hot.astype(F32), axis=0, keepdims=True).astype(jnp.int32)
    shift = side.bit_length() - 1
    owner_y, owner_x = owner >> shift, owner & (side - 1)
    odd = (owner_y + owner_x) & 1
    place = jnp.where(
        odd == 0,
        owner_y * group + (owner_x >> 1),
        banks // 2 + owner_x * group + (owner_y >> 1),
    )
    slot = place * most + standing
    placing[...] = (iota((banks * most, requests), 0) == slot).astype(BF16)
    local[3].wait()
    for copy in local[4:]:
        copy.start()
    packed[...] = (
        dot(placing[...], hidden_v[...]).astype(BF16).reshape(2 * side, chunk, half_model)
    )
    received[y] = packed[y]
    received[side + x] = packed[side + x]
    for p in range(side - 1):
        to_row(p, False, True)
    for p in range(side - 1):
        to_column(p)
    to_row(side - 1, True, True)
    to_column(side - 1)

    local[4].wait()
    local[5].wait()
    local[7].wait()
    wide = 2 * head
    key_parts = wk.shape[1] // wide

    def project_keys(n):
        at = n * wide
        raw = dot(images_v[...], wk_v[:, at : at + wide])
        for part in range(2):
            one = raw[:, part * head : (part + 1) * head]
            scale = lax.rsqrt(jnp.mean(one * one, axis=1, keepdims=True) + 1e-06)
            keys[:, :, at + part * head : at + (part + 1) * head] = (
                (one * scale * gain_v[...]).astype(BF16).reshape(tokens, ours, head)
            )

    def project_values(n):
        at = n * wide
        raw = dot(images_v[...], wv_v[:, at : at + wide])
        values[:, :, at : at + wide] = raw.astype(BF16).reshape(tokens, ours, wide)

    for part in range(2 * key_parts):
        if part == key_parts:
            local[6].wait()
        if part < key_parts:
            project_keys(part)
        else:
            project_values(part - key_parts)
    local[8].wait()

    lanes = tokens * BLOCK
    heads_each = (2 * half_query // head) // (wk.shape[1] // head)
    rows = heads_each * BLOCK
    token = iota((1, lanes), 1) // BLOCK
    tile = jnp.zeros((1, lanes), jnp.int32)
    for edge in range(TILE_TOKENS, tokens, TILE_TOKENS):
        tile = tile + (token >= edge).astype(jnp.int32)
    counts = jnp.broadcast_to(used_v[...].astype(F32), (8, ours)).astype(BF16)
    same = (iota((rows, lanes), 0) & (BLOCK - 1)) == (iota((rows, lanes), 1) & (BLOCK - 1))
    for b in range(ours // BLOCK):
        spread = (
            iota((ours, lanes), 0) == b * BLOCK + (iota((ours, lanes), 1) & (BLOCK - 1))
        ).astype(BF16)
        count = dot(counts, spread)[0:1]
        bias[b] = jnp.where(same & (tile.astype(F32) < count), 0.0, -1e30)

    slots = side * chunk
    in_slot = (iota((slots, group * rank), 0) & (chunk - 1)) // most
    keep = in_slot == iota((slots, group * rank), 1) // rank

    for kind, here in ((0, y), (1, x)):
        for slot_at in range(kind * group, (kind + 1) * group):

            @pl.when(own_slot != slot_at)
            def _(slot_at=slot_at):
                arrived(adapters.at[slot_at], adapter_send.at[0], adapter_recv.at[slot_at])

        for k in range(1, side):
            source = kind * side + (here + k) % side
            arrived(received.at[source], row_send.at[source], row_recv.at[source])
        low = dot(
            received[kind * side : (kind + 1) * side].reshape(slots, half_model),
            adapters[kind * group : (kind + 1) * group, :, :half_model].reshape(
                group * rank, half_model
            ),
            NT,
        )
        low_own[kind] = jnp.where(keep, low, 0.0)
        if kind == 0:

            @pl.when(core == 1)
            def _():
                pl.semaphore_wait(gate.at[2 * side], 1)

        start(low_own.at[kind], low_other.at[kind], low_send.at[kind], low_recv.at[kind], partner)
        arrived(low_other.at[kind], low_send.at[kind], low_recv.at[kind])
        low = (low_own[kind] + low_other[kind]).astype(BF16)
        result = dot(
            low,
            adapters[kind * group : (kind + 1) * group, :, half_model:].reshape(
                group * rank, half_query
            ),
        )
        raised[kind * side : (kind + 1) * side] = result.astype(BF16).reshape(
            side, chunk, half_query
        )
        returned[kind * side + here] = raised[kind * side + here]
        for distance in range(side // 2, 0, -1):
            for k in (distance, side - distance) if 2 * distance < side else (distance,):
                to = (here + k) % side
                start(
                    raised.at[kind * side + to],
                    returned.at[kind * side + here],
                    back_send.at[kind * side + to],
                    back_recv.at[kind * side + here],
                    {"aa": y * side + to} if kind else {"aa": to * side + x},
                )
    local[9].wait()
    for kind, here in ((0, y), (1, x)):
        for k in range(1, side):
            source = kind * side + (here + k) % side
            arrived(returned.at[source], back_send.at[k], back_recv.at[source])
    delta = dot(placing[...], returned[...].reshape(banks * most, half_query), TN)
    query = (base_v[...].astype(F32) + delta).astype(BF16)
    q_own[...] = query.reshape(2, ours, half_query)
    q_send[...] = q_own[1 - core]
    start(q_send, q_other, q_send_sem, q_recv_sem, partner)

    heads_kv = half_query // head // heads_each
    cells = [(b, g) for b in range(ours // BLOCK) for g in range(heads_kv)]

    def attend(q, part):
        first_kv = part * (heads_kv * head)
        for n, (b, g) in enumerate(cells):
            at = slice(b * BLOCK, (b + 1) * BLOCK)
            block = jnp.concatenate(
                [
                    q[at, (g * heads_each + i) * head : (g * heads_each + i + 1) * head]
                    for i in range(heads_each)
                ],
                axis=0,
            )
            key = keys[:, at, pl.ds(pl.multiple_of(first_kv + g * head, head), head)]
            scores[n] = (
                dot(block, key.reshape(lanes, head), NT) * (1.0 / math.sqrt(head)) + bias[b]
            )
        peaks = jnp.max(scores[...], axis=2, keepdims=True)
        weight = jnp.exp(scores[...] - peaks)
        totals[...] = jnp.broadcast_to(
            jnp.sum(weight, axis=2, keepdims=True), totals.shape
        )
        weights[...] = weight.astype(BF16)
        for n, (b, g) in enumerate(cells):
            at = slice(b * BLOCK, (b + 1) * BLOCK)
            value = values[:, at, pl.ds(pl.multiple_of(first_kv + g * head, head), head)]
            result = (dot(weights[n], value.reshape(lanes, head)) / totals[n]).astype(BF16)
            for i in range(heads_each):
                column = part * half_query + (g * heads_each + i) * head
                out[at, pl.ds(pl.multiple_of(column, head), head)] = result[
                    i * BLOCK : (i + 1) * BLOCK
                ]

    attend(q_own[core], core)
    arrived(q_other, q_send_sem, q_recv_sem)
    attend(q_other[...], 1 - core)
    own_at = (1 - parity) * x + parity * y
    for k in range(1, side):
        left(adapters.at[own_slot], adapter_send.at[(own_at + k) % side], adapter_recv.at[0])
    for kind, here in ((0, y), (1, x)):
        for k in range(1, side):
            at = kind * side + (here + k) % side
            left(packed.at[at], row_send.at[at], row_recv.at[at])
            left(raised.at[at], back_send.at[at], back_recv.at[at])
        left(low_own.at[kind], low_send.at[kind], low_recv.at[kind])
    left(q_send, q_send_sem, q_recv_sem)


def on_device(
    side,
    images,
    key_projection,
    value_projection,
    key_norm_gain,
    hidden,
    shared_query_base,
    adapter_down_matrix,
    adapter_up_matrix,
    tenant_adapter_index,
    used_tile_count,
):
    ours, tokens, model = images.shape
    requests, half_model = hidden.shape
    half_query = shared_query_base.shape[1]
    head = key_norm_gain.shape[0]
    kvw = key_projection.shape[1]
    banks = side * side
    most = 2 * requests // banks
    group = side // 2
    chunk = group * most
    rank = adapter_up_matrix.shape[1]
    heads_each = 2 * half_query // kvw
    cells = ours // BLOCK * (half_query // head // heads_each)
    args = (
        jnp.transpose(images, (1, 0, 2)).reshape(tokens * ours, model),
        key_projection,
        value_projection,
        key_norm_gain.reshape(1, head),
        hidden,
        shared_query_base,
        jnp.transpose(adapter_down_matrix[0]),
        adapter_up_matrix[0],
        tenant_adapter_index.reshape(1, requests),
        used_tile_count.reshape(1, ours),
    )
    dma = pltpu.SemaphoreType.DMA
    return pl.pallas_call(
        functools.partial(kernel, side, most),
        out_shape=jax.ShapeDtypeStruct((ours, 2 * half_query), BF16),
        in_specs=[pl.BlockSpec(memory_space=pl.ANY)] * len(args),
        out_specs=pl.BlockSpec(memory_space=pltpu.VMEM),
        scratch_shapes=[
            pltpu.VMEM((tokens * ours, model), BF16),
            pltpu.VMEM((model, kvw), BF16),
            pltpu.VMEM((model, kvw), BF16),
            pltpu.VMEM((1, head), F32),
            pltpu.VMEM((requests, half_model), BF16),
            pltpu.VMEM((requests, half_query), BF16),
            pltpu.VMEM((1, requests), jnp.int32),
            pltpu.VMEM((1, ours), jnp.int32),
            pltpu.VMEM((side, rank, half_model + half_query), BF16),
            pltpu.VMEM((2 * side, chunk, half_model), BF16),
            pltpu.VMEM((banks * most, requests), BF16),
            pltpu.VMEM((2 * side, chunk, half_model), BF16),
            pltpu.VMEM((2, side * chunk, group * rank), F32),
            pltpu.VMEM((2, side * chunk, group * rank), F32),
            pltpu.VMEM((2 * side, chunk, half_query), BF16),
            pltpu.VMEM((2 * side, chunk, half_query), BF16),
            pltpu.VMEM((2, ours, half_query), BF16),
            pltpu.VMEM((ours, half_query), BF16),
            pltpu.VMEM((ours, half_query), BF16),
            pltpu.VMEM((tokens, ours, kvw), BF16),
            pltpu.VMEM((tokens, ours, kvw), BF16),
            pltpu.VMEM((ours // BLOCK, heads_each * BLOCK, tokens * BLOCK), F32),
            pltpu.VMEM((cells, heads_each * BLOCK, tokens * BLOCK), F32),
            pltpu.VMEM((cells, heads_each * BLOCK, tokens * BLOCK), BF16),
            pltpu.VMEM((cells, heads_each * BLOCK, head), F32),
            pltpu.SemaphoreType.REGULAR((2 * side + 1,)),
            dma((10,)),
            dma((side,)),
            dma((side,)),
            dma((2 * side,)),
            dma((2 * side,)),
            dma((2 * side,)),
            dma((2 * side,)),
            dma((2,)),
            dma((2,)),
            dma(()),
            dma(()),
        ],
        compiler_params=pltpu.CompilerParams(collective_id=0, has_side_effects=True),
        name="adapter_attention",
    )(*args)


def solution(mesh):
    placed = (
        P(("ga", "aa", "ba"), None, None),
        P(),
        P(),
        P(),
        P(("ga", "aa"), "ba"),
        P(("ga", "aa"), "ba"),
        P("aa", None, None),
        P("aa", None, None),
        P(("ga", "aa"), None),
        P(("ga", "aa", "ba")),
    )
    return jax.shard_map(
        functools.partial(on_device, math.isqrt(mesh.shape["aa"])),
        mesh=mesh,
        in_specs=placed,
        out_specs=P(("ga", "aa", "ba"), None),
        check_vma=False,
    )
```

```python
import functools
import math

import jax
import jax.numpy as jnp
from jax import lax
from jax.experimental import pallas as pl
from jax.experimental.pallas import tpu as pltpu
from jax.sharding import PartitionSpec as P

TILE_TOKENS = 3
BLOCK = 16
MESH = pl.DeviceIdType.MESH
F32 = jnp.float32
BF16 = jnp.bfloat16
NT = (((1,), (1,)), ((), ()))
TN = (((0,), (0,)), ((), ()))


def dot(a, b, dims=(((1,), (0,)), ((), ()))):
    return lax.dot_general(a, b, dims, preferred_element_type=F32)


def iota(shape, dim):
    return lax.broadcasted_iota(jnp.int32, shape, dim)


def kernel(
    side,
    most,
    images,
    wk,
    wv,
    gain,
    hidden,
    base,
    down,
    up,
    ids,
    used,
    out,
    images_v,
    wk_v,
    wv_v,
    gain_v,
    hidden_v,
    base_v,
    ids_v,
    used_v,
    adapters,
    packed,
    placing,
    received,
    low_own,
    low_other,
    raised,
    returned,
    q_own,
    q_send,
    q_other,
    keys,
    values,
    bias,
    scores,
    weights,
    totals,
    gate,
    local_sem,
    adapter_send,
    adapter_recv,
    row_send,
    row_recv,
    back_send,
    back_recv,
    low_send,
    low_recv,
    q_send_sem,
    q_recv_sem,
):
    me = lax.axis_index("aa")
    core = lax.axis_index("ba")
    y, x = me // side, me % side
    partner = {"ba": 1 - core}
    parity = (y + x) % 2
    banks = side * side
    group = side // 2
    chunk = group * most
    requests, half_model = hidden.shape
    half_query = base.shape[1]
    rank = up.shape[0]
    tokens, ours = keys.shape[0], keys.shape[1]
    head = gain.shape[1]

    own_slot = (1 - parity) * (x // 2) + parity * (group + y // 2)

    def rank_of(index):
        return (index + banks - 1 + core) % banks

    mine = rank_of(me)
    last_column = jnp.where((core == 0) & (x == 0), 1, 0)
    last_row = jnp.where((core == 0) & (y == 0), 1, 0)
    around = [
        (index, gate_at, own_gate)
        for k in range(1, side)
        for index, gate_at, own_gate in (
            ((y + k) % side * side + x, (y + k) % side, y),
            (y * side + (x + k) % side, side + (x + k) % side, side + x),
        )
    ]

    barrier = pltpu.get_barrier_semaphore()
    pl.semaphore_signal(barrier, inc=1, device_id={"aa": me}, device_id_type=MESH)
    earlier_peers = 2 - core
    for index, gate_at, own_gate in around:
        earlier_peers = earlier_peers + jnp.where(rank_of(index) < mine, 1, 0)

        @pl.when(rank_of(index) > mine)
        def _(index=index):
            pl.semaphore_signal(barrier, inc=1, device_id={"aa": index}, device_id_type=MESH)

    @pl.when(core == 1)
    def _():
        pl.semaphore_signal(barrier, inc=1, device_id=partner, device_id_type=MESH)

    model_at = pl.multiple_of(core * half_model, half_model)
    query_at = pl.multiple_of(core * half_query, half_query)
    own_down = adapters.at[own_slot, :, pl.ds(0, half_model)]
    own_up = adapters.at[own_slot, :, pl.ds(half_model, half_query)]
    pairs = (
        (down.at[:, pl.ds(model_at, half_model)], own_down),
        (up.at[:, pl.ds(query_at, half_query)], own_up),
        (ids, ids_v),
        (hidden, hidden_v),
        (images, images_v),
        (wk, wk_v),
        (wv, wv_v),
        (gain, gain_v),
        (used, used_v),
        (base, base_v),
    )
    local = [pltpu.make_async_copy(s, d, local_sem.at[i]) for i, (s, d) in enumerate(pairs)]
    for copy in local[:4]:
        copy.start()

    def start(source, target, send_sem, recv_sem, device):
        pltpu.make_async_remote_copy(
            src_ref=source,
            dst_ref=target,
            send_sem=send_sem,
            recv_sem=recv_sem,
            device_id=device,
            device_id_type=MESH,
        ).start()

    def left(ref, send_sem, recv_sem):
        pltpu.make_async_remote_copy(
            src_ref=ref,
            dst_ref=ref,
            send_sem=send_sem,
            recv_sem=recv_sem,
            device_id=partner,
            device_id_type=MESH,
        ).wait_send()

    def arrived(ref, send_sem, recv_sem):
        pltpu.make_async_remote_copy(
            src_ref=ref,
            dst_ref=ref,
            send_sem=send_sem,
            recv_sem=recv_sem,
            device_id=partner,
            device_id_type=MESH,
        ).wait_recv()

    def to_row(p, adapter, rows):
        at = (p + last_row) % side
        index = y * side + at

        @pl.when(at != x)
        def _():
            if adapter:

                @pl.when(rank_of(index) > mine)
                def _():
                    pl.semaphore_wait(gate.at[side + at], 1)

                @pl.when(parity == 0)
                def _():
                    start(
                        adapters.at[own_slot],
                        adapters.at[own_slot],
                        adapter_send.at[at],
                        adapter_recv.at[own_slot],
                        {"aa": index},
                    )

            if rows:
                start(
                    packed.at[side + at],
                    received.at[side + x],
                    row_send.at[side + at],
                    row_recv.at[side + x],
                    {"aa": index},
                )

    def to_column(p):
        at = (p + last_column) % side
        index = at * side + x

        @pl.when(at != y)
        def _():
            @pl.when(rank_of(index) > mine)
            def _():
                pl.semaphore_wait(gate.at[at], 1)

            @pl.when(parity == 1)
            def _():
                start(
                    adapters.at[own_slot],
                    adapters.at[own_slot],
                    adapter_send.at[at],
                    adapter_recv.at[own_slot],
                    {"aa": index},
                )

            start(
                packed.at[at],
                received.at[y],
                row_send.at[at],
                row_recv.at[y],
                {"aa": index},
            )

    pl.semaphore_wait(barrier, earlier_peers)
    for index, gate_at, own_gate in around:

        @pl.when(rank_of(index) < mine)
        def _(index=index, own_gate=own_gate):
            pl.semaphore_signal(
                gate.at[own_gate], inc=1, device_id={"aa": index}, device_id_type=MESH
            )

    @pl.when(core == 0)
    def _():
        pl.semaphore_signal(gate.at[2 * side], inc=1, device_id=partner, device_id_type=MESH)

    local[0].wait()
    local[1].wait()
    for p in range(side - 1):
        to_row(p, True, False)

    local[2].wait()
    owner = ids_v[...]
    hot = (iota((banks, requests), 0) == owner).astype(BF16)
    earlier = (iota((requests, requests), 0) < iota((requests, requests), 1)).astype(BF16)
    before = dot(hot, earlier)
    standing = jnp.sum(before * hot.astype(F32), axis=0, keepdims=True).astype(jnp.int32)
    shift = side.bit_length() - 1
    owner_y, owner_x = owner >> shift, owner & (side - 1)
    odd = (owner_y + owner_x) & 1
    place = jnp.where(
        odd == 0,
        owner_y * group + (owner_x >> 1),
        banks // 2 + owner_x * group + (owner_y >> 1),
    )
    slot = place * most + standing
    placing[...] = (iota((banks * most, requests), 0) == slot).astype(BF16)
    local[3].wait()
    for copy in local[4:]:
        copy.start()
    packed[...] = (
        dot(placing[...], hidden_v[...]).astype(BF16).reshape(2 * side, chunk, half_model)
    )
    received[y] = packed[y]
    received[side + x] = packed[side + x]
    for p in range(side - 1):
        to_row(p, False, True)
    for p in range(side - 1):
        to_column(p)
    to_row(side - 1, True, True)
    to_column(side - 1)

    local[4].wait()
    local[5].wait()
    local[7].wait()
    wide = 2 * head
    key_parts = wk.shape[1] // wide

    def project_keys(n):
        at = n * wide
        raw = dot(images_v[...], wk_v[:, at : at + wide])
        for part in range(2):
            one = raw[:, part * head : (part + 1) * head]
            scale = lax.rsqrt(jnp.mean(one * one, axis=1, keepdims=True) + 1e-06)
            keys[:, :, at + part * head : at + (part + 1) * head] = (
                (one * scale * gain_v[...]).astype(BF16).reshape(tokens, ours, head)
            )

    def project_values(n):
        at = n * wide
        raw = dot(images_v[...], wv_v[:, at : at + wide])
        values[:, :, at : at + wide] = raw.astype(BF16).reshape(tokens, ours, wide)

    for part in range(key_parts):
        project_keys(part)
    local[8].wait()

    lanes = tokens * BLOCK
    heads_each = (2 * half_query // head) // (wk.shape[1] // head)
    rows = heads_each * BLOCK
    token = iota((1, lanes), 1) // BLOCK
    tile = jnp.zeros((1, lanes), jnp.int32)
    for edge in range(TILE_TOKENS, tokens, TILE_TOKENS):
        tile = tile + (token >= edge).astype(jnp.int32)
    counts = jnp.broadcast_to(used_v[...].astype(F32), (8, ours)).astype(BF16)
    same = (iota((rows, lanes), 0) & (BLOCK - 1)) == (iota((rows, lanes), 1) & (BLOCK - 1))
    for b in range(ours // BLOCK):
        spread = (
            iota((ours, lanes), 0) == b * BLOCK + (iota((ours, lanes), 1) & (BLOCK - 1))
        ).astype(BF16)
        count = dot(counts, spread)[0:1]
        bias[b] = jnp.where(same & (tile.astype(F32) < count), 0.0, -1e30)

    slots = side * chunk
    in_slot = (iota((slots, group * rank), 0) & (chunk - 1)) // most
    keep = in_slot == iota((slots, group * rank), 1) // rank

    for kind, here in ((0, y), (1, x)):
        for slot_at in range(kind * group, (kind + 1) * group):

            @pl.when(own_slot != slot_at)
            def _(slot_at=slot_at):
                arrived(adapters.at[slot_at], adapter_send.at[0], adapter_recv.at[slot_at])

        for k in range(1, side):
            source = kind * side + (here + k) % side
            arrived(received.at[source], row_send.at[source], row_recv.at[source])
        low = dot(
            received[kind * side : (kind + 1) * side].reshape(slots, half_model),
            adapters[kind * group : (kind + 1) * group, :, :half_model].reshape(
                group * rank, half_model
            ),
            NT,
        )
        low_own[kind] = jnp.where(keep, low, 0.0)
        if kind == 0:

            @pl.when(core == 1)
            def _():
                pl.semaphore_wait(gate.at[2 * side], 1)

        start(low_own.at[kind], low_other.at[kind], low_send.at[kind], low_recv.at[kind], partner)
        arrived(low_other.at[kind], low_send.at[kind], low_recv.at[kind])
        low = (low_own[kind] + low_other[kind]).astype(BF16)
        result = dot(
            low,
            adapters[kind * group : (kind + 1) * group, :, half_model:].reshape(
                group * rank, half_query
            ),
        )
        raised[kind * side : (kind + 1) * side] = result.astype(BF16).reshape(
            side, chunk, half_query
        )
        returned[kind * side + here] = raised[kind * side + here]
        for distance in range(side // 2, 0, -1):
            for k in (distance, side - distance) if 2 * distance < side else (distance,):
                to = (here + k) % side
                start(
                    raised.at[kind * side + to],
                    returned.at[kind * side + here],
                    back_send.at[kind * side + to],
                    back_recv.at[kind * side + here],
                    {"aa": y * side + to} if kind else {"aa": to * side + x},
                )
    local[6].wait()
    for part in range(key_parts):
        project_values(part)
    local[9].wait()
    for kind, here in ((0, y), (1, x)):
        for k in range(1, side):
            source = kind * side + (here + k) % side
            arrived(returned.at[source], back_send.at[k], back_recv.at[source])
    delta = dot(placing[...], returned[...].reshape(banks * most, half_query), TN)
    query = (base_v[...].astype(F32) + delta).astype(BF16)
    q_own[...] = query.reshape(2, ours, half_query)
    q_send[...] = q_own[1 - core]
    start(q_send, q_other, q_send_sem, q_recv_sem, partner)

    heads_kv = half_query // head // heads_each
    cells = [(b, g) for b in range(ours // BLOCK) for g in range(heads_kv)]

    def attend(q, part):
        first_kv = part * (heads_kv * head)
        for n, (b, g) in enumerate(cells):
            at = slice(b * BLOCK, (b + 1) * BLOCK)
            block = jnp.concatenate(
                [
                    q[at, (g * heads_each + i) * head : (g * heads_each + i + 1) * head]
                    for i in range(heads_each)
                ],
                axis=0,
            )
            key = keys[:, at, pl.ds(pl.multiple_of(first_kv + g * head, head), head)]
            scores[n] = (
                dot(block, key.reshape(lanes, head), NT) * (1.0 / math.sqrt(head)) + bias[b]
            )
        peaks = jnp.max(scores[...], axis=2, keepdims=True)
        weight = jnp.exp(scores[...] - peaks)
        totals[...] = jnp.broadcast_to(
            jnp.sum(weight, axis=2, keepdims=True), totals.shape
        )
        weights[...] = weight.astype(BF16)
        for n, (b, g) in enumerate(cells):
            at = slice(b * BLOCK, (b + 1) * BLOCK)
            value = values[:, at, pl.ds(pl.multiple_of(first_kv + g * head, head), head)]
            result = (dot(weights[n], value.reshape(lanes, head)) / totals[n]).astype(BF16)
            for i in range(heads_each):
                column = part * half_query + (g * heads_each + i) * head
                out[at, pl.ds(pl.multiple_of(column, head), head)] = result[
                    i * BLOCK : (i + 1) * BLOCK
                ]

    attend(q_own[core], core)
    arrived(q_other, q_send_sem, q_recv_sem)
    attend(q_other[...], 1 - core)
    own_at = (1 - parity) * x + parity * y
    for k in range(1, side):
        left(adapters.at[own_slot], adapter_send.at[(own_at + k) % side], adapter_recv.at[0])
    for kind, here in ((0, y), (1, x)):
        for k in range(1, side):
            at = kind * side + (here + k) % side
            left(packed.at[at], row_send.at[at], row_recv.at[at])
            left(raised.at[at], back_send.at[at], back_recv.at[at])
        left(low_own.at[kind], low_send.at[kind], low_recv.at[kind])
    left(q_send, q_send_sem, q_recv_sem)


def on_device(
    side,
    images,
    key_projection,
    value_projection,
    key_norm_gain,
    hidden,
    shared_query_base,
    adapter_down_matrix,
    adapter_up_matrix,
    tenant_adapter_index,
    used_tile_count,
):
    ours, tokens, model = images.shape
    requests, half_model = hidden.shape
    half_query = shared_query_base.shape[1]
    head = key_norm_gain.shape[0]
    kvw = key_projection.shape[1]
    banks = side * side
    most = 2 * requests // banks
    group = side // 2
    chunk = group * most
    rank = adapter_up_matrix.shape[1]
    heads_each = 2 * half_query // kvw
    cells = ours // BLOCK * (half_query // head // heads_each)
    args = (
        jnp.transpose(images, (1, 0, 2)).reshape(tokens * ours, model),
        key_projection,
        value_projection,
        key_norm_gain.reshape(1, head),
        hidden,
        shared_query_base,
        jnp.transpose(adapter_down_matrix[0]),
        adapter_up_matrix[0],
        tenant_adapter_index.reshape(1, requests),
        used_tile_count.reshape(1, ours),
    )
    dma = pltpu.SemaphoreType.DMA
    return pl.pallas_call(
        functools.partial(kernel, side, most),
        out_shape=pltpu.VMEM((ours, 2 * half_query), BF16),
        in_specs=[pl.BlockSpec(memory_space=pl.ANY)] * len(args),
        out_specs=pl.BlockSpec(memory_space=pltpu.VMEM),
        scratch_shapes=[
            pltpu.VMEM((tokens * ours, model), BF16),
            pltpu.VMEM((model, kvw), BF16),
            pltpu.VMEM((model, kvw), BF16),
            pltpu.VMEM((1, head), F32),
            pltpu.VMEM((requests, half_model), BF16),
            pltpu.VMEM((requests, half_query), BF16),
            pltpu.VMEM((1, requests), jnp.int32),
            pltpu.VMEM((1, ours), jnp.int32),
            pltpu.VMEM((side, rank, half_model + half_query), BF16),
            pltpu.VMEM((2 * side, chunk, half_model), BF16),
            pltpu.VMEM((banks * most, requests), BF16),
            pltpu.VMEM((2 * side, chunk, half_model), BF16),
            pltpu.VMEM((2, side * chunk, group * rank), F32),
            pltpu.VMEM((2, side * chunk, group * rank), F32),
            pltpu.VMEM((2 * side, chunk, half_query), BF16),
            pltpu.VMEM((2 * side, chunk, half_query), BF16),
            pltpu.VMEM((2, ours, half_query), BF16),
            pltpu.VMEM((ours, half_query), BF16),
            pltpu.VMEM((ours, half_query), BF16),
            pltpu.VMEM((tokens, ours, kvw), BF16),
            pltpu.VMEM((tokens, ours, kvw), BF16),
            pltpu.VMEM((ours // BLOCK, heads_each * BLOCK, tokens * BLOCK), F32),
            pltpu.VMEM((cells, heads_each * BLOCK, tokens * BLOCK), F32),
            pltpu.VMEM((cells, heads_each * BLOCK, tokens * BLOCK), BF16),
            pltpu.VMEM((cells, heads_each * BLOCK, head), F32),
            pltpu.SemaphoreType.REGULAR((2 * side + 1,)),
            dma((10,)),
            dma((side,)),
            dma((side,)),
            dma((2 * side,)),
            dma((2 * side,)),
            dma((2 * side,)),
            dma((2 * side,)),
            dma((2,)),
            dma((2,)),
            dma(()),
            dma(()),
        ],
        compiler_params=pltpu.CompilerParams(collective_id=0, has_side_effects=True),
        name="adapter_attention",
    )(*args)


def solution(mesh):
    placed = (
        P(("ga", "aa", "ba"), None, None),
        P(),
        P(),
        P(),
        P(("ga", "aa"), "ba"),
        P(("ga", "aa"), "ba"),
        P("aa", None, None),
        P("aa", None, None),
        P(("ga", "aa"), None),
        P(("ga", "aa", "ba")),
    )
    return jax.shard_map(
        functools.partial(on_device, math.isqrt(mesh.shape["aa"])),
        mesh=mesh,
        in_specs=placed,
        out_specs=P(("ga", "aa", "ba"), None),
        check_vma=False,
    )
```
